32 devices in a mesh: groups: 2 (over x), seq: 16 (over z, y, core).
Axes of the slice: x: 2, y: 2, z: 4, core: 2. Of those that a mesh axis runs over, the one named last changes fastest.
Arguments:
- attn_query: bfloat16 [8192, 2048], P(('groups', 'seq')), parts along dimension 0, may hold values from -16 to 16
- attn_key: bfloat16 [8192, 2048], P(('groups', 'seq')), parts along dimension 0, may hold values from -16 to 16
- attn_value: bfloat16 [8192, 2048], P(('groups', 'seq')), parts along dimension 0, may hold values from -6 to 6
- mesa_query: bfloat16 [8192, 2048], P(('groups', 'seq')), parts along dimension 0, may hold values from -6 to 6
- mesa_key: bfloat16 [8192, 2048], P(('groups', 'seq')), parts along dimension 0, may hold values from -16 to 16
- log_decay: float32 [8192, 16], P(('groups', 'seq')), parts along dimension 0, may hold values from -1 to 0
- input_gate: float32 [8192, 16], P(('groups', 'seq')), parts along dimension 0, may hold values from 0.2 to 1
- regularizer: float32 [16, 128], replicated, may hold values from 0.5 to 4
Outputs:
- attention: bfloat16 [8192, 2048], P(('groups', 'seq')), parts along dimension 0
- mesa_out: bfloat16 [8192, 2048], P(('groups', 'seq')), parts along dimension 0
The draws below stay inside these ranges and needn't reach their ends.
There are 2 independent parts, one for each index of `groups`. The reference program is written for one: setup_inputs(seed, part) draws one part's arguments, and reference() takes and returns one part's arrays. A program takes and returns all parts, laid end to end along the dimension named above; an argument that names none is the same for every part. Nothing has to cross between parts.
All inputs are finite; a program needn't handle non-finite values.
Results may differ from the reference program's by a relative error of at most 0.017.
Values may be sent and summed in bfloat16 or wider, within the bound.
A program may use at most 128 MiB of HBM per device.

```python
import math
import jax
import jax.numpy as jnp
from jax import lax

HEAD_GROUP = 16
DK = 128
FEATURES = 2048
WINDOW = 2048
SPAN = 64
CG_ITERS = 8
TOK_DEV = 256
TOKEN_LENGTH = 4096


def drawn_pair(key):
    random_seeds = jax.random.split(jax.random.fold_in(key, 11), 2)
    base_query = jnp.clip(jax.random.normal(random_seeds[0], (TOKEN_LENGTH, FEATURES), jnp.float32), -4.0, 4.0)
    base_key = jnp.clip(jax.random.normal(random_seeds[1], (TOKEN_LENGTH, FEATURES), jnp.float32), -4.0, 4.0)
    return (base_query, base_key)


def draw_attn_query(key, part):
    return drawn_pair(key)[0].astype(jnp.bfloat16)


def draw_attn_key(key, part):
    return drawn_pair(key)[1].astype(jnp.bfloat16)


def draw_mesa_key(key, part):
    random_seeds = jax.random.split(jax.random.fold_in(key, 29), 3)
    overall = math.sqrt(32.0 / TOKEN_LENGTH)
    entries = jnp.clip(jax.random.normal(random_seeds[0], (TOKEN_LENGTH, FEATURES), jnp.float32), -4.0, 4.0)
    column = jnp.exp(jax.random.uniform(random_seeds[1], (1, FEATURES), jnp.float32, math.log(0.3), math.log(1.5)))
    coarse_result = jax.random.uniform(random_seeds[2], (TOKEN_LENGTH, 1), jnp.float32, 0.5, 1.5)
    return (entries * column * coarse_result * overall).astype(jnp.bfloat16)


def draw_log_decay(key, part):
    random_seeds = jax.random.split(jax.random.fold_in(key, 37), 7)
    share = 0.5
    slow = jax.random.uniform(random_seeds[0], (HEAD_GROUP,), jnp.float32) < share
    slow_rate = jax.random.uniform(random_seeds[1], (HEAD_GROUP,), jnp.float32, 0.1, 0.25) * math.log(10.0) / TOKEN_LENGTH
    fast_rate = math.log(10.0) / jax.random.uniform(random_seeds[2], (HEAD_GROUP,), jnp.float32, 30.0, 50.0)
    head_decay_rate = jnp.where(slow, slow_rate, fast_rate)
    slab_factor = jnp.exp(jax.random.uniform(random_seeds[3], (TOKEN_LENGTH // TOK_DEV, HEAD_GROUP), jnp.float32, math.log(0.5), math.log(2.0)))
    piece_rows = jnp.repeat(slab_factor, TOK_DEV, axis=0)
    coarse_result = jax.random.uniform(random_seeds[4], (TOKEN_LENGTH, HEAD_GROUP), jnp.float32, 0.5, 1.5)
    segment_list = jax.random.randint(random_seeds[5], (2,), 0, TOKEN_LENGTH)
    segment_rows = jnp.any(jnp.arange(TOKEN_LENGTH)[:, None] == segment_list[None, :], axis=1)[:, None]
    segment_loss = jnp.log(jax.random.uniform(random_seeds[6], (1, HEAD_GROUP), jnp.float32, 0.5, 0.8))
    return -(head_decay_rate[None, :] * piece_rows * coarse_result) + jnp.where(segment_rows, segment_loss, 0.0)


def block_scale(rng, shape, cuts, smallest, largest):
    loudness, own = 1.0, jax.random.fold_in(rng, 6)
    for position, shards_of in cuts:
        draws = jnp.exp(jax.random.uniform(jax.random.fold_in(own, position), (shards_of,), jnp.float32, smallest / len(cuts), largest / len(cuts)))
        loudness = loudness * jnp.repeat(draws, shape[position] // shards_of).reshape([-1 if axis == position else 1 for axis in range(len(shape))])
    return loudness


def scatter_about(rng, extent, deviation, bound, cuts=(), kind=jnp.bfloat16):
    level = block_scale(rng, extent, cuts, -0.22, 0.18) if cuts else 1.0
    values = jax.random.normal(rng, extent, jnp.float32) * deviation * level
    return jnp.minimum(jnp.maximum(values, -bound), bound).astype(kind)


def setup_inputs(seed: int = 0, part: int = 0) -> dict:
    arg_keys = jax.random.split(jax.random.key(seed), 9)
    part_splits = jax.random.split(jax.random.fold_in(arg_keys[8], part), 9)
    attn_query = draw_attn_query(jax.random.fold_in(jax.random.fold_in(arg_keys[8], part), 71), part)
    attn_key = draw_attn_key(jax.random.fold_in(jax.random.fold_in(arg_keys[8], part), 71), part)
    attn_value = scatter_about(part_splits[2], (TOKEN_LENGTH, FEATURES), 1.0, 6.0, ((0, 16),))
    mesa_query = scatter_about(part_splits[3], (TOKEN_LENGTH, FEATURES), 1.0, 6.0, ((0, 16),))
    mesa_key = draw_mesa_key(jax.random.fold_in(jax.random.fold_in(arg_keys[8], part), 71), part)
    log_decay = draw_log_decay(jax.random.fold_in(jax.random.fold_in(arg_keys[8], part), 71), part)
    input_gate = jnp.clip(0.2 + 0.8 * jax.random.uniform(part_splits[6], (TOKEN_LENGTH, HEAD_GROUP), jnp.float32) ** block_scale(part_splits[6], (TOKEN_LENGTH, HEAD_GROUP), ((0, 16),), -0.2, 0.2), 0.2, 1.0)
    regularizer = jnp.clip(jnp.exp(jax.random.uniform(arg_keys[7], (HEAD_GROUP, DK), jnp.float32, math.log(0.5), math.log(4.0))), 0.5, 4.0)
    return {"attn_query": attn_query, "attn_key": attn_key, "attn_value": attn_value, "mesa_query": mesa_query, "mesa_key": mesa_key, "log_decay": log_decay, "input_gate": input_gate, "regularizer": regularizer}


exact_mode = lax.Precision.HIGHEST
masked_score = -1e30


def span_update(states, inputs, ridge_diag):
    gram_start, cross_start = states
    queries, key_rows, value_rows, log_rates, gate_rows = inputs
    q_heads = jnp.transpose(queries, (1, 0, 2))
    k_heads = jnp.transpose(key_rows, (1, 0, 2))
    v_heads = jnp.transpose(value_rows, (1, 0, 2))
    cumulative = jnp.transpose(jnp.cumsum(log_rates, axis=0))
    length = cumulative.shape[1]
    causal = (jnp.arange(length)[:, None] >= jnp.arange(length)[None, :])[None]
    distance = cumulative[:, :, None] - cumulative[:, None, :]
    decay_mix = jnp.where(causal, jnp.exp(jnp.where(causal, distance, 0.0)), 0.0) * jnp.transpose(gate_rows)[:, None, :]
    start_scale = jnp.exp(cumulative)[:, :, None]

    def operator_apply(search):
        carried = start_scale * jnp.einsum('hcd,hed->hce', search, gram_start, precision=exact_mode)
        products = jnp.einsum('hjd,hid->hji', search, k_heads, precision=exact_mode)
        local_part = jnp.einsum('hji,hid->hjd', decay_mix * products, k_heads, precision=exact_mode)
        return carried + local_part + ridge_diag[:, None, :] * search

    iterate = jnp.zeros_like(q_heads)
    remain = q_heads
    search = q_heads
    norm_now = jnp.sum(remain * remain, axis=-1, keepdims=True)
    for sweep_index in range(CG_ITERS):
        image_vec = operator_apply(search)
        step_size = norm_now / (jnp.sum(search * image_vec, axis=-1, keepdims=True) + 1e-6)
        iterate = iterate + step_size * search
        remain = remain - step_size * image_vec
        norm_next = jnp.sum(remain * remain, axis=-1, keepdims=True)
        search = remain + (norm_next / (norm_now + 1e-6)) * search
        norm_now = norm_next
    products = jnp.einsum('hjd,hid->hji', iterate, k_heads, precision=exact_mode)
    mesa_rows = start_scale * jnp.einsum('hje,hde->hjd', iterate, cross_start, precision=exact_mode)
    mesa_rows = mesa_rows + jnp.einsum('hji,hid->hjd', decay_mix * products, v_heads, precision=exact_mode)
    tail_weight = (jnp.exp(cumulative[:, -1:] - cumulative) * jnp.transpose(gate_rows))[:, :, None]
    end_scale = jnp.exp(cumulative[:, -1])[:, None, None]
    gram_end = end_scale * gram_start + jnp.einsum('hid,hie->hde', k_heads * tail_weight, k_heads, precision=exact_mode)
    cross_end = end_scale * cross_start + jnp.einsum('hid,hie->hde', v_heads * tail_weight, k_heads, precision=exact_mode)
    return (gram_end, cross_end), jnp.transpose(mesa_rows, (1, 0, 2))


def mesa_pass(queries, key_rows, value_rows, log_rates, gate_rows, ridge_diag, gram_start, cross_start):
    row_total = queries.shape[0]
    span_count = row_total // SPAN

    def shaped(array_in):
        return array_in.reshape((span_count, SPAN) + array_in.shape[1:])

    def advance(states, inputs):
        return span_update(states, inputs, ridge_diag)

    finished, outputs = lax.scan(advance, (gram_start, cross_start),
                                 (shaped(queries), shaped(key_rows), shaped(value_rows), shaped(log_rates), shaped(gate_rows)))
    return outputs.reshape(row_total, -1)


def reference(attn_query, attn_key, attn_value, mesa_query, mesa_key, log_decay, input_gate, regularizer):
    head_count, head_size = regularizer.shape
    total_rows = attn_query.shape[0]
    block_rows = TOK_DEV
    block_count = total_rows // block_rows
    queries = attn_query.reshape(block_count, block_rows, head_count, head_size)
    padded_keys = jnp.pad(attn_key, ((WINDOW, 0), (0, 0)))
    padded_values = jnp.pad(attn_value, ((WINDOW, 0), (0, 0)))
    scale_factor = head_size ** -0.5

    def attend(inputs):
        block_index, block_queries = inputs
        first_row = (block_index * block_rows).astype(jnp.int32)
        key_rows = lax.dynamic_slice_in_dim(padded_keys, first_row, WINDOW + block_rows, 0).reshape(-1, head_count, head_size)
        value_rows = lax.dynamic_slice_in_dim(padded_values, first_row, WINDOW + block_rows, 0).reshape(-1, head_count, head_size)
        scores = jnp.einsum('qhd,khd->hqk', block_queries.astype(jnp.float32), key_rows.astype(jnp.float32)) * scale_factor
        query_pos = first_row + jnp.arange(block_rows, dtype=jnp.int32)[:, None]
        key_pos = first_row - WINDOW + jnp.arange(WINDOW + block_rows, dtype=jnp.int32)[None, :]
        distance = query_pos - key_pos
        inside = ((distance >= 0) & (distance < WINDOW) & (key_pos >= 0))[None]
        scores = jnp.where(inside, scores, masked_score)
        row_max = jnp.max(scores, axis=-1, keepdims=True)
        weights = jnp.exp(scores - row_max) * inside.astype(jnp.float32)
        rounded = weights.astype(jnp.bfloat16)
        summed = jnp.einsum('hqk,khd->hqd', rounded.astype(jnp.float32), value_rows.astype(jnp.float32))
        normed = summed / jnp.sum(weights, axis=-1, keepdims=True)
        return jnp.transpose(normed, (1, 0, 2)).reshape(block_rows, -1).astype(jnp.bfloat16)

    attention = lax.map(attend, (jnp.arange(block_count, dtype=jnp.int32), queries)).reshape(total_rows, -1)
    shape3 = (total_rows, head_count, head_size)
    gram_zero = jnp.zeros((head_count, head_size, head_size), jnp.float32)
    mesa_out = mesa_pass(mesa_query.astype(jnp.float32).reshape(shape3), mesa_key.astype(jnp.float32).reshape(shape3),
                         attention.astype(jnp.float32).reshape(shape3), log_decay, input_gate, regularizer,
                         gram_zero, gram_zero)
    return attention, mesa_out.astype(jnp.bfloat16)
```

```python
import jax
import jax.numpy as jnp
from jax import lax
from jax.experimental import pallas as pl
from jax.experimental.pallas import tpu as pltpu
from jax.sharding import PartitionSpec as P
import functools
import math

WINDOW = 2048
SPAN = 64
CG_ITERS = 8


exact_mode = lax.Precision.HIGHEST
masked_score = -1e30


def prefix(shard, axis, join, neutral):
    place = lax.axis_index(axis)
    gathered = jax.tree.map(
        lambda a, kind: lax.all_gather(a.astype(kind), axis), shard, (jnp.bfloat16, jnp.bfloat16)
    )
    state = jax.tree.map(lambda a, e: jnp.zeros_like(a) + jnp.asarray(e, a.dtype), shard, neutral)

    def one(lap, state):
        return join(
            state,
            jax.tree.map(
                lambda a, own: lax.dynamic_index_in_dim(a, lap, 0, False).astype(own.dtype),
                gathered,
                shard,
            ),
        )

    return lax.fori_loop(0, place, one, state)


def passed_along(value, axis, steps):
    count = lax.axis_size(axis)
    first, last = (max(0, -steps), min(count, count - steps))
    return lax.ppermute(value, axis, [(source, source + steps) for source in range(first, last)])


def span_update(states, inputs, ridge_diag):
    gram_start, cross_start = states
    queries, key_rows, value_rows, log_rates, gate_rows = inputs
    q_heads = jnp.transpose(queries, (1, 0, 2))
    k_heads = jnp.transpose(key_rows, (1, 0, 2))
    v_heads = jnp.transpose(value_rows, (1, 0, 2))
    cumulative = jnp.transpose(jnp.cumsum(log_rates, axis=0))
    length = cumulative.shape[1]
    causal = (jnp.arange(length)[:, None] >= jnp.arange(length)[None, :])[None]
    distance = cumulative[:, :, None] - cumulative[:, None, :]
    decay_mix = (
        jnp.where(causal, jnp.exp(jnp.where(causal, distance, 0.0)), 0.0)
        * jnp.transpose(gate_rows)[:, None, :]
    )
    start_scale = jnp.exp(cumulative)[:, :, None]
    iterate = jnp.zeros_like(q_heads)
    remain = q_heads
    search = q_heads
    norm_now = jnp.sum(remain * remain, axis=-1, keepdims=True)
    for sweep_index in range(CG_ITERS):
        carried = start_scale * jnp.einsum("hcd,hed->hce", search, gram_start, precision=exact_mode)
        operator_products = jnp.einsum("hjd,hid->hji", search, k_heads, precision=exact_mode)
        local_part = jnp.einsum(
            "hji,hid->hjd", decay_mix * operator_products, k_heads, precision=exact_mode
        )
        image_vec = carried + local_part + ridge_diag[:, None, :] * search
        step_size = norm_now / (jnp.sum(search * image_vec, axis=-1, keepdims=True) + 1e-06)
        iterate = iterate + step_size * search
        remain = remain - step_size * image_vec
        norm_next = jnp.sum(remain * remain, axis=-1, keepdims=True)
        search = remain + norm_next / (norm_now + 1e-06) * search
        norm_now = norm_next
    products = jnp.einsum("hjd,hid->hji", iterate, k_heads, precision=exact_mode)
    mesa_rows = start_scale * jnp.einsum("hje,hde->hjd", iterate, cross_start, precision=exact_mode)
    mesa_rows = mesa_rows + jnp.einsum(
        "hji,hid->hjd", decay_mix * products, v_heads, precision=exact_mode
    )
    tail_weight = (jnp.exp(cumulative[:, -1:] - cumulative) * jnp.transpose(gate_rows))[:, :, None]
    end_scale = jnp.exp(cumulative[:, -1])[:, None, None]
    gram_end = end_scale * gram_start + jnp.einsum(
        "hid,hie->hde", k_heads * tail_weight, k_heads, precision=exact_mode
    )
    cross_end = end_scale * cross_start + jnp.einsum(
        "hid,hie->hde", v_heads * tail_weight, k_heads, precision=exact_mode
    )
    return ((gram_end, cross_end), jnp.transpose(mesa_rows, (1, 0, 2)))


def mesa_pass(
    queries, key_rows, value_rows, log_rates, gate_rows, ridge_diag, gram_start, cross_start
):
    row_total = queries.shape[0]
    span_count = row_total // SPAN

    def shaped(array_in):
        return array_in.reshape((span_count, SPAN) + array_in.shape[1:])

    def advance(states, inputs):
        return span_update(states, inputs, ridge_diag)

    finished, outputs = lax.scan(
        advance,
        (gram_start, cross_start),
        (
            shaped(queries),
            shaped(key_rows),
            shaped(value_rows),
            shaped(log_rates),
            shaped(gate_rows),
        ),
    )
    return outputs.reshape(row_total, -1)


def fold_block(state_now, queries, key_value, query_first, key_first):
    running_max, running_sum, weighted = state_now
    row_count, head_count, head_size = queries.shape
    key_rows = key_value[0].reshape(-1, head_count, head_size)
    value_rows = key_value[1].reshape(-1, head_count, head_size)
    scores = jnp.einsum(
        "qhd,khd->hqk", queries, key_rows, preferred_element_type=jnp.float32
    ) * head_size ** (-0.5)
    query_pos = query_first + jnp.arange(row_count, dtype=jnp.int32)[:, None]
    key_pos = key_first + jnp.arange(key_rows.shape[0], dtype=jnp.int32)[None, :]
    distance = query_pos - key_pos
    inside = ((distance >= 0) & (distance < WINDOW) & (key_pos >= 0))[None]
    scores = jnp.where(inside, scores, masked_score)
    new_max = jnp.maximum(running_max, jnp.max(scores, axis=-1))
    weights = jnp.exp(scores - new_max[:, :, None]) * inside.astype(jnp.float32)
    rescale = jnp.exp(running_max - new_max)
    running_sum = running_sum * rescale + jnp.sum(weights, axis=-1)
    weighted = weighted * rescale[:, :, None] + jnp.einsum(
        "hqk,khd->hqd", weights.astype(jnp.bfloat16), value_rows, preferred_element_type=jnp.float32
    )
    return (new_max, running_sum, weighted)


def combine_pair(earlier, later):
    return (earlier[0] + later[0], jnp.exp(later[0])[:, None, None] * earlier[1] + later[1])


def slab_body(
    attn_query, attn_key, attn_value, mesa_query, mesa_key, log_decay, input_gate, regularizer
):
    row_count = attn_query.shape[0]
    head_count, head_size = regularizer.shape
    shape3 = (row_count, head_count, head_size)
    slab_first = lax.axis_index("seq") * row_count
    keys_float = mesa_key.astype(jnp.float32).reshape(shape3)
    slab_log = jnp.sum(log_decay, axis=0)
    tail_log = slab_log[None, :] - jnp.cumsum(log_decay, axis=0)
    weight_rows = (jnp.exp(tail_log) * input_gate)[:, :, None]
    gram_local = jnp.einsum(
        "lhd,lhe->hde", keys_float * weight_rows, keys_float, precision=exact_mode
    )
    zero_log = jnp.zeros_like(slab_log)
    zero_state = jnp.zeros_like(gram_local)
    gram_prefix = prefix((slab_log, gram_local), "seq", combine_pair, (zero_log, zero_state))[1]
    queries = attn_query.reshape(shape3)
    key_value = jnp.stack([attn_key, attn_value])
    state_now = (
        jnp.full((head_count, row_count), masked_score, jnp.float32),
        jnp.zeros((head_count, row_count), jnp.float32),
        jnp.zeros((head_count, row_count, head_size), jnp.float32),
    )
    state_now = fold_block(state_now, queries, key_value, slab_first, slab_first)
    reach = -(-WINDOW // row_count)
    moving = key_value
    for hop_index in range(1, reach + 1):
        moving = passed_along(moving, "seq", 1)
        state_now = fold_block(
            state_now, queries, moving, slab_first, slab_first - hop_index * row_count
        )
    normed = state_now[2] / state_now[1][:, :, None]
    attention = jnp.transpose(normed, (1, 0, 2)).reshape(row_count, -1).astype(jnp.bfloat16)
    values_float = attention.astype(jnp.float32).reshape(shape3)
    cross_local = jnp.einsum(
        "lhd,lhe->hde", values_float * weight_rows, keys_float, precision=exact_mode
    )
    cross_prefix = prefix((slab_log, cross_local), "seq", combine_pair, (zero_log, zero_state))[1]
    mesa_out = mesa_pass(
        mesa_query.astype(jnp.float32).reshape(shape3),
        keys_float,
        values_float,
        log_decay,
        input_gate,
        regularizer,
        gram_prefix,
        cross_prefix,
    )
    return (attention, mesa_out.astype(jnp.bfloat16))


CHUNK = 128
WAYS = 4
BF16 = jnp.bfloat16
F32 = jnp.float32
NT = (((1,), (1,)), ((), ()))
TN = (((0,), (0,)), ((), ()))


def dot(a, b, dims=None):
    if dims is None:
        return jnp.dot(a, b, preferred_element_type=F32)
    return lax.dot_general(a, b, dims, preferred_element_type=F32)


def two_terms(a):
    high = a.astype(BF16)
    low = (a - high.astype(F32)).astype(BF16)
    return jnp.concatenate([high, low], axis=1)


def attend_block(q_ref, k_ref, v_ref, out_ref, i, first, count, rows, banded):
    scale = math.log2(math.e) / math.sqrt(q_ref.shape[1])
    queries = q_ref[pl.ds(pl.multiple_of(i * rows, rows), rows), :]
    base = pl.multiple_of(first * rows, rows)
    row = lax.broadcasted_iota(jnp.int32, (rows, rows), 0)
    col = lax.broadcasted_iota(jnp.int32, (rows, rows), 1)
    scores, top = [], None
    for j in range(count):
        s = dot(queries, k_ref[pl.ds(base + j * rows, rows), :], NT)
        if banded and j == 0:
            s = jnp.where(row - col + (count - 1) * rows < WINDOW, s, masked_score)
        if j == count - 1 or (not banded and j == count - 2):
            s = jnp.where(row - col + (i - first - j) * rows >= 0, s, masked_score)
        scores.append(s)
        top = s if top is None else jnp.maximum(top, s)
    top = jnp.max(top, axis=1, keepdims=True)
    total, weights = None, []
    for s in scores:
        w = jnp.exp2((s - top) * scale)
        total = w if total is None else total + w
        weights.append(w.astype(BF16))
    total = jnp.sum(total, axis=1, keepdims=True)
    summed = dot(
        jnp.concatenate(weights, axis=1), v_ref[pl.ds(base, count * rows), :]
    )
    out_ref[pl.ds(pl.multiple_of(i * rows, rows), rows), :] = (summed / total).astype(BF16)


def attend_all(q_ref, k_ref, v_ref, out_ref, rows):
    blocks = q_ref.shape[0] // rows
    reach = WINDOW // rows
    early = min(reach, blocks)
    for low in range(0, early, 2):
        high = min(low + 2, early)

        def one(i, carry, high=high):
            attend_block(q_ref, k_ref, v_ref, out_ref, i, 0, high, rows, False)
            return carry

        lax.fori_loop(low, high, one, 0)
    if blocks > reach:

        def late(i, carry):
            attend_block(
                q_ref, k_ref, v_ref, out_ref, i, i - reach, reach + 1, rows, True
            )
            return carry

        lax.fori_loop(reach, blocks, late, 0)


def span(c):
    return pl.ds(pl.multiple_of(c * CHUNK, CHUNK), CHUNK)


def column_form(row):
    return jnp.transpose(jnp.broadcast_to(row, (CHUNK, CHUNK)))


def tail_keys(k_ref, cum_ref, gate_ref, c):
    cum, gate = cum_ref[pl.ds(c, 1), :], gate_ref[pl.ds(c, 1), :]
    weight = column_form(jnp.exp(cum[:, CHUNK - 1 :] - cum) * gate)
    keys = k_ref[span(c), :]
    return (keys.astype(F32) * weight).astype(BF16), jnp.exp(cum[:, CHUNK - 1 :])


def mix_of(cum_ref, gate_ref, c):
    cum, gate = cum_ref[pl.ds(c, 1), :], gate_ref[pl.ds(c, 1), :]
    col = column_form(cum)
    shape = (CHUNK, CHUNK)
    causal = lax.broadcasted_iota(jnp.int32, shape, 0) >= lax.broadcasted_iota(
        jnp.int32, shape, 1
    )
    mix = jnp.exp(jnp.where(causal, col - cum, masked_score)) * gate
    return mix, jnp.exp(col)


def gram_states(k_ref, other_ref, cum_ref, gate_ref, starts_ref):
    chunks = cum_ref.shape[0]

    def step(g, state):
        for w in range(WAYS):
            c = g * WAYS + w
            starts_ref[c] = state.astype(BF16)
            keys, end = tail_keys(k_ref, cum_ref, gate_ref, c)
            state = end * state + dot(keys, other_ref[span(c), :], TN)
        return state

    lax.fori_loop(0, chunks // WAYS, step, jnp.zeros((CHUNK, CHUNK), F32))


def solve_all(q_ref, k_ref, cum_ref, gate_ref, ridge_ref, gram_ref, x_ref):
    ridge = ridge_ref[...]
    chunks = cum_ref.shape[0]

    def group(g, carry):
        ids = [g * WAYS + w for w in range(WAYS)]
        mixes = [mix_of(cum_ref, gate_ref, c) for c in ids]
        keys = [k_ref[span(c), :] for c in ids]
        grams = [gram_ref[c] for c in ids]
        sides = [
            jnp.concatenate(
                [jnp.concatenate([a, a], axis=1), jnp.concatenate([k, k], axis=1)], axis=0
            )
            for a, k in zip(grams, keys)
        ]
        stacks = [jnp.concatenate([k, k], axis=0) for k in keys]
        state = []
        for c in ids:
            q = q_ref[span(c), :].astype(F32)
            state.append((jnp.zeros_like(q), q, q, jnp.sum(q * q, axis=1, keepdims=True)))

        def sweep(n, state):
            both = [dot(two_terms(s[2]), side, NT) for s, side in zip(state, sides)]
            local = [
                dot(two_terms(m[0] * b[:, CHUNK:]), k) for m, b, k in zip(mixes, both, stacks)
            ]
            out = []
            for (x, r, p, rr), b, l, m in zip(state, both, local, mixes):
                a = m[1] * b[:, :CHUNK] + l + ridge * p
                alpha = rr / (jnp.sum(p * a, axis=1, keepdims=True) + 1e-6)
                x = x + alpha * p
                r = r - alpha * a
                new = jnp.sum(r * r, axis=1, keepdims=True)
                p = r + (new / (rr + 1e-6)) * p
                out.append((x, r, p, new))
            return tuple(out)

        state = lax.fori_loop(0, CG_ITERS, sweep, tuple(state))
        for c, s in zip(ids, state):
            x_ref[span(c), :] = s[0]
        return carry

    lax.fori_loop(0, chunks // WAYS, group, 0)


def read_out(k_ref, v_ref, cum_ref, gate_ref, cross_ref, x_ref, out_ref):
    chunks = cum_ref.shape[0]

    def group(g, carry):
        for w in range(WAYS):
            c = g * WAYS + w
            mix, start = mix_of(cum_ref, gate_ref, c)
            keys, values, cross = k_ref[span(c), :], v_ref[span(c), :], cross_ref[c]
            x = two_terms(x_ref[span(c), :])
            products = dot(x, jnp.concatenate([keys, keys], axis=1), NT)
            rows = start * dot(x, jnp.concatenate([cross, cross], axis=0))
            rows = rows + dot(
                two_terms(mix * products), jnp.concatenate([values, values], axis=0)
            )
            out_ref[span(c), :] = rows.astype(BF16)
        return carry

    lax.fori_loop(0, chunks // WAYS, group, 0)


def head_kernel(
    rows, q, k, v, mq, mk, cum, gate, ridge, att, out, gram, cross, x
):
    attend_all(q, k, v, att, rows)
    gram_states(mk, mk, cum, gate, gram)
    solve_all(mq, mk, cum, gate, ridge, gram, x)
    gram_states(mk, att, cum, gate, cross)
    read_out(mk, att, cum, gate, cross, x, out)


def head_body(
    attn_query, attn_key, attn_value, mesa_query, mesa_key, log_decay, input_gate, regularizer
):
    rows = attn_query.shape[0]
    heads, size = regularizer.shape
    devices = lax.axis_size("seq")
    tokens = rows * devices

    def to_heads(a):
        return lax.all_to_all(a, "seq", 1, 0, tiled=True)

    q, k, v, mq, mk = (
        to_heads(a) for a in (attn_query, attn_key, attn_value, mesa_query, mesa_key)
    )
    rates = jnp.stack([jnp.transpose(log_decay), jnp.transpose(input_gate)], axis=1)
    rates = lax.all_to_all(rates, "seq", 0, 0, tiled=True)
    chunks = tokens // CHUNK
    cum = jnp.cumsum(rates[:, 0].reshape(chunks, CHUNK), axis=1)
    gate = rates[:, 1].reshape(chunks, CHUNK)
    ridge = lax.dynamic_slice_in_dim(regularizer, lax.axis_index("seq"), 1, 0)
    whole = jax.ShapeDtypeStruct((tokens, size), BF16)
    vmem = pl.BlockSpec(memory_space=pltpu.VMEM)
    att, out = pl.pallas_call(
        functools.partial(head_kernel, rows),
        out_shape=(whole, whole),
        in_specs=[vmem] * 8,
        out_specs=(vmem, vmem),
        scratch_shapes=[
            pltpu.VMEM((chunks, size, size), BF16),
            pltpu.VMEM((chunks, size, size), BF16),
            pltpu.VMEM((tokens, size), F32),
        ],
        compiler_params=pltpu.CompilerParams(vmem_limit_bytes=56 * 1024 * 1024),
    )(q, k, v, mq, mk, cum, gate, ridge)

    def to_slabs(a):
        return lax.all_to_all(a, "seq", 0, 1, tiled=True)

    return to_slabs(att), to_slabs(out)


def fits_heads(mesh, rows, heads, size):
    tokens = rows * mesh.shape["seq"]
    return (
        mesh.shape["seq"] == heads
        and size == CHUNK
        and WINDOW % rows == 0
        and tokens % (CHUNK * WAYS) == 0
    )


def solution(mesh):
    spec = P(("groups", "seq"), None)

    def body(*args):
        heads, size = args[7].shape
        chosen = head_body if fits_heads(mesh, args[0].shape[0], heads, size) else slab_body
        return chosen(*args)

    return jax.shard_map(
        body,
        mesh=mesh,
        in_specs=(spec,) * 7 + (P(),),
        out_specs=(spec, spec),
        check_vma=False,
    )
```

```python
import jax
import jax.numpy as jnp
from jax import lax
from jax.experimental import pallas as pl
from jax.experimental.pallas import tpu as pltpu
from jax.sharding import PartitionSpec as P
import functools
import math

WINDOW = 2048
SPAN = 64
CG_ITERS = 8


exact_mode = lax.Precision.HIGHEST
masked_score = -1e30


def prefix(shard, axis, join, neutral):
    place = lax.axis_index(axis)
    gathered = jax.tree.map(
        lambda a, kind: lax.all_gather(a.astype(kind), axis), shard, (jnp.bfloat16, jnp.bfloat16)
    )
    state = jax.tree.map(lambda a, e: jnp.zeros_like(a) + jnp.asarray(e, a.dtype), shard, neutral)

    def one(lap, state):
        return join(
            state,
            jax.tree.map(
                lambda a, own: lax.dynamic_index_in_dim(a, lap, 0, False).astype(own.dtype),
                gathered,
                shard,
            ),
        )

    return lax.fori_loop(0, place, one, state)


def passed_along(value, axis, steps):
    count = lax.axis_size(axis)
    first, last = (max(0, -steps), min(count, count - steps))
    return lax.ppermute(value, axis, [(source, source + steps) for source in range(first, last)])


def span_update(states, inputs, ridge_diag):
    gram_start, cross_start = states
    queries, key_rows, value_rows, log_rates, gate_rows = inputs
    q_heads = jnp.transpose(queries, (1, 0, 2))
    k_heads = jnp.transpose(key_rows, (1, 0, 2))
    v_heads = jnp.transpose(value_rows, (1, 0, 2))
    cumulative = jnp.transpose(jnp.cumsum(log_rates, axis=0))
    length = cumulative.shape[1]
    causal = (jnp.arange(length)[:, None] >= jnp.arange(length)[None, :])[None]
    distance = cumulative[:, :, None] - cumulative[:, None, :]
    decay_mix = (
        jnp.where(causal, jnp.exp(jnp.where(causal, distance, 0.0)), 0.0)
        * jnp.transpose(gate_rows)[:, None, :]
    )
    start_scale = jnp.exp(cumulative)[:, :, None]
    iterate = jnp.zeros_like(q_heads)
    remain = q_heads
    search = q_heads
    norm_now = jnp.sum(remain * remain, axis=-1, keepdims=True)
    for sweep_index in range(CG_ITERS):
        carried = start_scale * jnp.einsum("hcd,hed->hce", search, gram_start, precision=exact_mode)
        operator_products = jnp.einsum("hjd,hid->hji", search, k_heads, precision=exact_mode)
        local_part = jnp.einsum(
            "hji,hid->hjd", decay_mix * operator_products, k_heads, precision=exact_mode
        )
        image_vec = carried + local_part + ridge_diag[:, None, :] * search
        step_size = norm_now / (jnp.sum(search * image_vec, axis=-1, keepdims=True) + 1e-06)
        iterate = iterate + step_size * search
        remain = remain - step_size * image_vec
        norm_next = jnp.sum(remain * remain, axis=-1, keepdims=True)
        search = remain + norm_next / (norm_now + 1e-06) * search
        norm_now = norm_next
    products = jnp.einsum("hjd,hid->hji", iterate, k_heads, precision=exact_mode)
    mesa_rows = start_scale * jnp.einsum("hje,hde->hjd", iterate, cross_start, precision=exact_mode)
    mesa_rows = mesa_rows + jnp.einsum(
        "hji,hid->hjd", decay_mix * products, v_heads, precision=exact_mode
    )
    tail_weight = (jnp.exp(cumulative[:, -1:] - cumulative) * jnp.transpose(gate_rows))[:, :, None]
    end_scale = jnp.exp(cumulative[:, -1])[:, None, None]
    gram_end = end_scale * gram_start + jnp.einsum(
        "hid,hie->hde", k_heads * tail_weight, k_heads, precision=exact_mode
    )
    cross_end = end_scale * cross_start + jnp.einsum(
        "hid,hie->hde", v_heads * tail_weight, k_heads, precision=exact_mode
    )
    return ((gram_end, cross_end), jnp.transpose(mesa_rows, (1, 0, 2)))


def mesa_pass(
    queries, key_rows, value_rows, log_rates, gate_rows, ridge_diag, gram_start, cross_start
):
    row_total = queries.shape[0]
    span_count = row_total // SPAN

    def shaped(array_in):
        return array_in.reshape((span_count, SPAN) + array_in.shape[1:])

    def advance(states, inputs):
        return span_update(states, inputs, ridge_diag)

    finished, outputs = lax.scan(
        advance,
        (gram_start, cross_start),
        (
            shaped(queries),
            shaped(key_rows),
            shaped(value_rows),
            shaped(log_rates),
            shaped(gate_rows),
        ),
    )
    return outputs.reshape(row_total, -1)


def fold_block(state_now, queries, key_value, query_first, key_first):
    running_max, running_sum, weighted = state_now
    row_count, head_count, head_size = queries.shape
    key_rows = key_value[0].reshape(-1, head_count, head_size)
    value_rows = key_value[1].reshape(-1, head_count, head_size)
    scores = jnp.einsum(
        "qhd,khd->hqk", queries, key_rows, preferred_element_type=jnp.float32
    ) * head_size ** (-0.5)
    query_pos = query_first + jnp.arange(row_count, dtype=jnp.int32)[:, None]
    key_pos = key_first + jnp.arange(key_rows.shape[0], dtype=jnp.int32)[None, :]
    distance = query_pos - key_pos
    inside = ((distance >= 0) & (distance < WINDOW) & (key_pos >= 0))[None]
    scores = jnp.where(inside, scores, masked_score)
    new_max = jnp.maximum(running_max, jnp.max(scores, axis=-1))
    weights = jnp.exp(scores - new_max[:, :, None]) * inside.astype(jnp.float32)
    rescale = jnp.exp(running_max - new_max)
    running_sum = running_sum * rescale + jnp.sum(weights, axis=-1)
    weighted = weighted * rescale[:, :, None] + jnp.einsum(
        "hqk,khd->hqd", weights.astype(jnp.bfloat16), value_rows, preferred_element_type=jnp.float32
    )
    return (new_max, running_sum, weighted)


def combine_pair(earlier, later):
    return (earlier[0] + later[0], jnp.exp(later[0])[:, None, None] * earlier[1] + later[1])


def slab_body(
    attn_query, attn_key, attn_value, mesa_query, mesa_key, log_decay, input_gate, regularizer
):
    row_count = attn_query.shape[0]
    head_count, head_size = regularizer.shape
    shape3 = (row_count, head_count, head_size)
    slab_first = lax.axis_index("seq") * row_count
    keys_float = mesa_key.astype(jnp.float32).reshape(shape3)
    slab_log = jnp.sum(log_decay, axis=0)
    tail_log = slab_log[None, :] - jnp.cumsum(log_decay, axis=0)
    weight_rows = (jnp.exp(tail_log) * input_gate)[:, :, None]
    gram_local = jnp.einsum(
        "lhd,lhe->hde", keys_float * weight_rows, keys_float, precision=exact_mode
    )
    zero_log = jnp.zeros_like(slab_log)
    zero_state = jnp.zeros_like(gram_local)
    gram_prefix = prefix((slab_log, gram_local), "seq", combine_pair, (zero_log, zero_state))[1]
    queries = attn_query.reshape(shape3)
    key_value = jnp.stack([attn_key, attn_value])
    state_now = (
        jnp.full((head_count, row_count), masked_score, jnp.float32),
        jnp.zeros((head_count, row_count), jnp.float32),
        jnp.zeros((head_count, row_count, head_size), jnp.float32),
    )
    state_now = fold_block(state_now, queries, key_value, slab_first, slab_first)
    reach = -(-WINDOW // row_count)
    moving = key_value
    for hop_index in range(1, reach + 1):
        moving = passed_along(moving, "seq", 1)
        state_now = fold_block(
            state_now, queries, moving, slab_first, slab_first - hop_index * row_count
        )
    normed = state_now[2] / state_now[1][:, :, None]
    attention = jnp.transpose(normed, (1, 0, 2)).reshape(row_count, -1).astype(jnp.bfloat16)
    values_float = attention.astype(jnp.float32).reshape(shape3)
    cross_local = jnp.einsum(
        "lhd,lhe->hde", values_float * weight_rows, keys_float, precision=exact_mode
    )
    cross_prefix = prefix((slab_log, cross_local), "seq", combine_pair, (zero_log, zero_state))[1]
    mesa_out = mesa_pass(
        mesa_query.astype(jnp.float32).reshape(shape3),
        keys_float,
        values_float,
        log_decay,
        input_gate,
        regularizer,
        gram_prefix,
        cross_prefix,
    )
    return (attention, mesa_out.astype(jnp.bfloat16))


CHUNK = 128
WAYS = 4
BF16 = jnp.bfloat16
F32 = jnp.float32
NT = (((1,), (1,)), ((), ()))
TN = (((0,), (0,)), ((), ()))


def dot(a, b, dims=None):
    if dims is None:
        return jnp.dot(a, b, preferred_element_type=F32)
    return lax.dot_general(a, b, dims, preferred_element_type=F32)


def two_terms(a):
    high = a.astype(BF16)
    low = (a - high.astype(F32)).astype(BF16)
    return jnp.concatenate([high, low], axis=1)


def attend_block(q_ref, k_ref, v_ref, out_ref, i, first, count, rows, banded):
    scale = math.log2(math.e) / math.sqrt(q_ref.shape[1])
    queries = q_ref[pl.ds(pl.multiple_of(i * rows, rows), rows), :]
    base = pl.multiple_of(first * rows, rows)
    row = lax.broadcasted_iota(jnp.int32, (rows, rows), 0)
    col = lax.broadcasted_iota(jnp.int32, (rows, rows), 1)
    scores, top = [], None
    for j in range(count):
        s = dot(queries, k_ref[pl.ds(base + j * rows, rows), :], NT)
        if banded and j == 0:
            s = jnp.where(row - col + (count - 1) * rows < WINDOW, s, masked_score)
        if j == count - 1 or (not banded and j == count - 2):
            s = jnp.where(row - col + (i - first - j) * rows >= 0, s, masked_score)
        scores.append(s)
        top = s if top is None else jnp.maximum(top, s)
    top = jnp.max(top, axis=1, keepdims=True)
    total, weights = None, []
    for s in scores:
        w = jnp.exp2((s - top) * scale)
        total = w if total is None else total + w
        weights.append(w.astype(BF16))
    total = jnp.sum(total, axis=1, keepdims=True)
    summed = dot(
        jnp.concatenate(weights, axis=1), v_ref[pl.ds(base, count * rows), :]
    )
    out_ref[pl.ds(pl.multiple_of(i * rows, rows), rows), :] = (summed / total).astype(BF16)


def attend_all(q_ref, k_ref, v_ref, out_ref, rows, done):
    blocks = q_ref.shape[0] // rows
    reach = WINDOW // rows
    early = min(reach, blocks)
    for low in range(0, early, 2):
        high = min(low + 2, early)

        def one(i, carry, high=high):
            attend_block(q_ref, k_ref, v_ref, out_ref, i, 0, high, rows, False)
            done(i)
            return carry

        lax.fori_loop(low, high, one, 0)
    if blocks > reach:

        def late(i, carry):
            attend_block(
                q_ref, k_ref, v_ref, out_ref, i, i - reach, reach + 1, rows, True
            )
            done(i)
            return carry

        lax.fori_loop(reach, blocks, late, 0)


def flat(c, per):
    return c[0] * per + c[1]


def span(c, per):
    return pl.ds(pl.multiple_of(flat(c, per) * CHUNK, CHUNK), CHUNK)


def chunk_ids(g, per, ways=WAYS):
    slabs = ways // per
    return [(g * slabs + w // per, w % per) for w in range(ways)]


def column_form(row):
    return jnp.transpose(jnp.broadcast_to(row, (CHUNK, CHUNK)))


def rates_of(rates_ref, c):
    slab, place = c
    per = rates_ref.shape[1] // 4
    return rates_ref[slab, place : place + 1, :], rates_ref[slab, per + place : per + place + 1, :]


def tail_keys(k_ref, rates_ref, c, per):
    cum, gate = rates_of(rates_ref, c)
    weight = column_form(jnp.exp(cum[:, CHUNK - 1 :] - cum) * gate)
    keys = k_ref[span(c, per), :]
    return (keys.astype(F32) * weight).astype(BF16), jnp.exp(cum[:, CHUNK - 1 :])


def mix_of(rates_ref, c):
    cum, gate = rates_of(rates_ref, c)
    col = column_form(cum)
    shape = (CHUNK, CHUNK)
    causal = lax.broadcasted_iota(jnp.int32, shape, 0) >= lax.broadcasted_iota(
        jnp.int32, shape, 1
    )
    mix = jnp.exp(jnp.where(causal, col - cum, masked_score)) * gate
    return mix, jnp.exp(col)


def gram_states(k_ref, other_ref, rates_ref, starts_ref):
    per = rates_ref.shape[1] // 4
    chunks = rates_ref.shape[0] * per

    def step(g, state):
        for c in chunk_ids(g, per):
            starts_ref[flat(c, per)] = state.astype(BF16)
            keys, end = tail_keys(k_ref, rates_ref, c, per)
            state = end * state + dot(keys, other_ref[span(c, per), :], TN)
        return state

    lax.fori_loop(0, chunks // WAYS, step, jnp.zeros((CHUNK, CHUNK), F32))


def solve_all(q_ref, k_ref, rates_ref, ridge_ref, gram_ref, x_ref):
    ridge = ridge_ref
    per = rates_ref.shape[1] // 4
    chunks = rates_ref.shape[0] * per

    def group(g, carry):
        ids = chunk_ids(g, per)
        mixes = [mix_of(rates_ref, c) for c in ids]
        keys = [k_ref[span(c, per), :] for c in ids]
        grams = [gram_ref[flat(c, per)] for c in ids]
        sides = [
            jnp.concatenate(
                [jnp.concatenate([a, a], axis=1), jnp.concatenate([k, k], axis=1)], axis=0
            )
            for a, k in zip(grams, keys)
        ]
        stacks = [jnp.concatenate([k, k], axis=0) for k in keys]
        state = []
        for c in ids:
            q = q_ref[span(c, per), :].astype(F32)
            state.append((jnp.zeros_like(q), q, q, jnp.sum(q * q, axis=1, keepdims=True)))

        def sweep(n, state):
            both = [dot(two_terms(s[2]), side, NT) for s, side in zip(state, sides)]
            local = [
                dot(two_terms(m[0] * b[:, CHUNK:]), k) for m, b, k in zip(mixes, both, stacks)
            ]
            out = []
            for (x, r, p, rr), b, l, m in zip(state, both, local, mixes):
                a = m[1] * b[:, :CHUNK] + l + ridge * p
                alpha = rr / (jnp.sum(p * a, axis=1, keepdims=True) + 1e-6)
                x = x + alpha * p
                r = r - alpha * a
                new = jnp.sum(r * r, axis=1, keepdims=True)
                p = r + (new / (rr + 1e-6)) * p
                out.append((x, r, p, new))
            return tuple(out)

        state = lax.fori_loop(0, CG_ITERS, sweep, tuple(state))
        for c, s in zip(ids, state):
            x_ref[span(c, per), :] = s[0]
        return carry

    lax.fori_loop(0, chunks // WAYS, group, 0)


def read_out(k_ref, v_ref, rates_ref, cross_ref, x_ref, out_ref, slab):
    per = rates_ref.shape[1] // 4
    for c in chunk_ids(slab, per, per):
        mix, start = mix_of(rates_ref, c)
        keys, values, cross = k_ref[span(c, per), :], v_ref[span(c, per), :], cross_ref[flat(c, per)]
        x = two_terms(x_ref[span(c, per), :])
        products = dot(x, jnp.concatenate([keys, keys], axis=1), NT)
        rows = start * dot(x, jnp.concatenate([cross, cross], axis=0))
        rows = rows + dot(two_terms(mix * products), jnp.concatenate([values, values], axis=0))
        out_ref[span(c, per), :] = rows.astype(BF16)


def head_kernel(n, *refs):
    ins, rates_in, ridge_in = refs[:5], refs[5], refs[6]
    results = refs[7:9]
    bufs, rates, homes = refs[9:14], refs[14], refs[15:17]
    gram, cross, x = refs[17:20]
    send, recv, own = refs[20:23]
    q, k, v, mk, mq = bufs
    att, out = homes
    rows, size = ins[0].shape[0], ridge_in.shape[1]
    group, me = lax.axis_index("groups"), lax.axis_index("seq")

    def row_block(ref, s):
        return ref.at[pl.ds(pl.multiple_of(s * rows, rows), rows), :]

    def col_block(ref, h):
        return ref.at[:, pl.ds(pl.multiple_of(h * size, size), size)]

    def ends(a, source, target):
        if a < 5:
            return col_block(ins[a], target), row_block(bufs[a], source)
        if a == 5:
            return rates_in.at[target], rates.at[source]
        return row_block(homes[a - 6], target), col_block(results[a - 6], source)

    def remote(a, source, target, peer):
        src, dst = ends(a, source, target)
        return pltpu.make_async_remote_copy(
            src_ref=src,
            dst_ref=dst,
            send_sem=send.at[a, target],
            recv_sem=recv.at[a, source],
            device_id=(group, peer),
            device_id_type=pl.DeviceIdType.MESH,
        )

    def local(a):
        src, dst = ends(a, me, me)
        return pltpu.make_async_copy(src, dst, own.at[a])

    def other(t):
        return lax.rem(me + t, n)

    def over_peers(act):
        def one(t, carry):
            act(other(t))
            return carry

        lax.fori_loop(1, n, one, 0)

    def arrive(a):
        over_peers(lambda peer: remote(a, peer, me, peer).wait_recv())
        local(a).wait()

    def give(a, slab):
        @pl.when(slab != me)
        def _():
            remote(a, me, slab, slab).start()

        @pl.when(slab == me)
        def _():
            local(a).start()

    barrier = pltpu.get_barrier_semaphore()
    over_peers(
        lambda peer: pl.semaphore_signal(
            barrier, inc=1, device_id=(group, peer), device_id_type=pl.DeviceIdType.MESH
        )
    )
    pl.semaphore_wait(barrier, n - 1)
    for a in SEND_ORDER:
        over_peers(lambda peer: remote(a, me, peer, peer).start())
        local(a).start()

    for a in (0, 1, 2):
        arrive(a)
    attend_all(q, k, v, att, rows, lambda i: give(6, i))
    for a in (5, 3, 4):
        arrive(a)
    gram_states(mk, mk, rates, gram)
    gram_states(mk, att, rates, cross)
    solve_all(mq, mk, rates, ridge_in[pl.ds(me, 1), :], gram, x)

    def slab_out(t, carry):
        slab = other(t + 1)
        read_out(mk, att, rates, cross, x, out, slab)
        give(7, slab)
        return carry

    lax.fori_loop(0, n, slab_out, 0)
    for a in (6, 7):
        arrive(a)
    for a in range(8):
        over_peers(lambda peer: remote(a, me, peer, peer).wait_send())


SEND_ORDER = (0, 1, 2, 5, 3, 4)


def head_body(
    attn_query, attn_key, attn_value, mesa_query, mesa_key, log_decay, input_gate, regularizer
):
    rows = attn_query.shape[0]
    heads, size = regularizer.shape
    devices = lax.axis_size("seq")
    tokens = rows * devices
    per, chunks = rows // CHUNK, tokens // CHUNK
    cum = jnp.cumsum(log_decay.reshape(per, CHUNK, heads), axis=1)
    rates = jnp.concatenate([cum, input_gate.reshape(per, CHUNK, heads)], axis=0)
    rates = jnp.pad(jnp.transpose(rates, (2, 0, 1)), ((0, 0), (0, 2 * per), (0, 0)))
    slab = jax.ShapeDtypeStruct((rows, heads * size), BF16)
    vmem = pl.BlockSpec(memory_space=pltpu.VMEM)
    anywhere = pl.BlockSpec(memory_space=pl.ANY)
    return pl.pallas_call(
        functools.partial(head_kernel, devices),
        out_shape=(slab, slab),
        in_specs=[anywhere] * 5 + [vmem] * 2,
        out_specs=(anywhere, anywhere),
        scratch_shapes=[pltpu.VMEM((tokens, size), BF16)] * 5
        + [pltpu.VMEM((devices, 4 * per, CHUNK), F32)]
        + [pltpu.VMEM((tokens, size), BF16)] * 2
        + [pltpu.VMEM((chunks, size, size), BF16)] * 2
        + [
            pltpu.VMEM((tokens, size), F32),
            pltpu.SemaphoreType.DMA((8, devices)),
            pltpu.SemaphoreType.DMA((8, devices)),
            pltpu.SemaphoreType.DMA((8,)),
        ],
        compiler_params=pltpu.CompilerParams(
            collective_id=0, has_side_effects=True, vmem_limit_bytes=56 * 1024 * 1024
        ),
    )(attn_query, attn_key, attn_value, mesa_key, mesa_query, rates, regularizer)


def fits_heads(mesh, rows, heads, size):
    tokens = rows * mesh.shape["seq"]
    return (
        mesh.shape["seq"] == heads
        and size == CHUNK
        and WINDOW % rows == 0
        and rows % CHUNK == 0
        and WAYS % (rows // CHUNK) == 0
        and tokens % (CHUNK * WAYS) == 0
    )


def solution(mesh):
    spec = P(("groups", "seq"), None)

    def body(*args):
        heads, size = args[7].shape
        chosen = head_body if fits_heads(mesh, args[0].shape[0], heads, size) else slab_body
        return chosen(*args)

    return jax.shard_map(
        body,
        mesh=mesh,
        in_specs=(spec,) * 7 + (P(),),
        out_specs=(spec, spec),
        check_vma=False,
    )
```

```python
import jax
import jax.numpy as jnp
from jax import lax
from jax.experimental import pallas as pl
from jax.experimental.pallas import tpu as pltpu
from jax.sharding import PartitionSpec as P
import functools
import math

WINDOW = 2048
SPAN = 64
CG_ITERS = 8


exact_mode = lax.Precision.HIGHEST
masked_score = -1e30


def prefix(shard, axis, join, neutral):
    place = lax.axis_index(axis)
    gathered = jax.tree.map(
        lambda a, kind: lax.all_gather(a.astype(kind), axis), shard, (jnp.bfloat16, jnp.bfloat16)
    )
    state = jax.tree.map(lambda a, e: jnp.zeros_like(a) + jnp.asarray(e, a.dtype), shard, neutral)

    def one(lap, state):
        return join(
            state,
            jax.tree.map(
                lambda a, own: lax.dynamic_index_in_dim(a, lap, 0, False).astype(own.dtype),
                gathered,
                shard,
            ),
        )

    return lax.fori_loop(0, place, one, state)


def passed_along(value, axis, steps):
    count = lax.axis_size(axis)
    first, last = (max(0, -steps), min(count, count - steps))
    return lax.ppermute(value, axis, [(source, source + steps) for source in range(first, last)])


def span_update(states, inputs, ridge_diag):
    gram_start, cross_start = states
    queries, key_rows, value_rows, log_rates, gate_rows = inputs
    q_heads = jnp.transpose(queries, (1, 0, 2))
    k_heads = jnp.transpose(key_rows, (1, 0, 2))
    v_heads = jnp.transpose(value_rows, (1, 0, 2))
    cumulative = jnp.transpose(jnp.cumsum(log_rates, axis=0))
    length = cumulative.shape[1]
    causal = (jnp.arange(length)[:, None] >= jnp.arange(length)[None, :])[None]
    distance = cumulative[:, :, None] - cumulative[:, None, :]
    decay_mix = (
        jnp.where(causal, jnp.exp(jnp.where(causal, distance, 0.0)), 0.0)
        * jnp.transpose(gate_rows)[:, None, :]
    )
    start_scale = jnp.exp(cumulative)[:, :, None]
    iterate = jnp.zeros_like(q_heads)
    remain = q_heads
    search = q_heads
    norm_now = jnp.sum(remain * remain, axis=-1, keepdims=True)
    for sweep_index in range(CG_ITERS):
        carried = start_scale * jnp.einsum("hcd,hed->hce", search, gram_start, precision=exact_mode)
        operator_products = jnp.einsum("hjd,hid->hji", search, k_heads, precision=exact_mode)
        local_part = jnp.einsum(
            "hji,hid->hjd", decay_mix * operator_products, k_heads, precision=exact_mode
        )
        image_vec = carried + local_part + ridge_diag[:, None, :] * search
        step_size = norm_now / (jnp.sum(search * image_vec, axis=-1, keepdims=True) + 1e-06)
        iterate = iterate + step_size * search
        remain = remain - step_size * image_vec
        norm_next = jnp.sum(remain * remain, axis=-1, keepdims=True)
        search = remain + norm_next / (norm_now + 1e-06) * search
        norm_now = norm_next
    products = jnp.einsum("hjd,hid->hji", iterate, k_heads, precision=exact_mode)
    mesa_rows = start_scale * jnp.einsum("hje,hde->hjd", iterate, cross_start, precision=exact_mode)
    mesa_rows = mesa_rows + jnp.einsum(
        "hji,hid->hjd", decay_mix * products, v_heads, precision=exact_mode
    )
    tail_weight = (jnp.exp(cumulative[:, -1:] - cumulative) * jnp.transpose(gate_rows))[:, :, None]
    end_scale = jnp.exp(cumulative[:, -1])[:, None, None]
    gram_end = end_scale * gram_start + jnp.einsum(
        "hid,hie->hde", k_heads * tail_weight, k_heads, precision=exact_mode
    )
    cross_end = end_scale * cross_start + jnp.einsum(
        "hid,hie->hde", v_heads * tail_weight, k_heads, precision=exact_mode
    )
    return ((gram_end, cross_end), jnp.transpose(mesa_rows, (1, 0, 2)))


def mesa_pass(
    queries, key_rows, value_rows, log_rates, gate_rows, ridge_diag, gram_start, cross_start
):
    row_total = queries.shape[0]
    span_count = row_total // SPAN

    def shaped(array_in):
        return array_in.reshape((span_count, SPAN) + array_in.shape[1:])

    def advance(states, inputs):
        return span_update(states, inputs, ridge_diag)

    finished, outputs = lax.scan(
        advance,
        (gram_start, cross_start),
        (
            shaped(queries),
            shaped(key_rows),
            shaped(value_rows),
            shaped(log_rates),
            shaped(gate_rows),
        ),
    )
    return outputs.reshape(row_total, -1)


def fold_block(state_now, queries, key_value, query_first, key_first):
    running_max, running_sum, weighted = state_now
    row_count, head_count, head_size = queries.shape
    key_rows = key_value[0].reshape(-1, head_count, head_size)
    value_rows = key_value[1].reshape(-1, head_count, head_size)
    scores = jnp.einsum(
        "qhd,khd->hqk", queries, key_rows, preferred_element_type=jnp.float32
    ) * head_size ** (-0.5)
    query_pos = query_first + jnp.arange(row_count, dtype=jnp.int32)[:, None]
    key_pos = key_first + jnp.arange(key_rows.shape[0], dtype=jnp.int32)[None, :]
    distance = query_pos - key_pos
    inside = ((distance >= 0) & (distance < WINDOW) & (key_pos >= 0))[None]
    scores = jnp.where(inside, scores, masked_score)
    new_max = jnp.maximum(running_max, jnp.max(scores, axis=-1))
    weights = jnp.exp(scores - new_max[:, :, None]) * inside.astype(jnp.float32)
    rescale = jnp.exp(running_max - new_max)
    running_sum = running_sum * rescale + jnp.sum(weights, axis=-1)
    weighted = weighted * rescale[:, :, None] + jnp.einsum(
        "hqk,khd->hqd", weights.astype(jnp.bfloat16), value_rows, preferred_element_type=jnp.float32
    )
    return (new_max, running_sum, weighted)


def combine_pair(earlier, later):
    return (earlier[0] + later[0], jnp.exp(later[0])[:, None, None] * earlier[1] + later[1])


def slab_body(
    attn_query, attn_key, attn_value, mesa_query, mesa_key, log_decay, input_gate, regularizer
):
    row_count = attn_query.shape[0]
    head_count, head_size = regularizer.shape
    shape3 = (row_count, head_count, head_size)
    slab_first = lax.axis_index("seq") * row_count
    keys_float = mesa_key.astype(jnp.float32).reshape(shape3)
    slab_log = jnp.sum(log_decay, axis=0)
    tail_log = slab_log[None, :] - jnp.cumsum(log_decay, axis=0)
    weight_rows = (jnp.exp(tail_log) * input_gate)[:, :, None]
    gram_local = jnp.einsum(
        "lhd,lhe->hde", keys_float * weight_rows, keys_float, precision=exact_mode
    )
    zero_log = jnp.zeros_like(slab_log)
    zero_state = jnp.zeros_like(gram_local)
    gram_prefix = prefix((slab_log, gram_local), "seq", combine_pair, (zero_log, zero_state))[1]
    queries = attn_query.reshape(shape3)
    key_value = jnp.stack([attn_key, attn_value])
    state_now = (
        jnp.full((head_count, row_count), masked_score, jnp.float32),
        jnp.zeros((head_count, row_count), jnp.float32),
        jnp.zeros((head_count, row_count, head_size), jnp.float32),
    )
    state_now = fold_block(state_now, queries, key_value, slab_first, slab_first)
    reach = -(-WINDOW // row_count)
    moving = key_value
    for hop_index in range(1, reach + 1):
        moving = passed_along(moving, "seq", 1)
        state_now = fold_block(
            state_now, queries, moving, slab_first, slab_first - hop_index * row_count
        )
    normed = state_now[2] / state_now[1][:, :, None]
    attention = jnp.transpose(normed, (1, 0, 2)).reshape(row_count, -1).astype(jnp.bfloat16)
    values_float = attention.astype(jnp.float32).reshape(shape3)
    cross_local = jnp.einsum(
        "lhd,lhe->hde", values_float * weight_rows, keys_float, precision=exact_mode
    )
    cross_prefix = prefix((slab_log, cross_local), "seq", combine_pair, (zero_log, zero_state))[1]
    mesa_out = mesa_pass(
        mesa_query.astype(jnp.float32).reshape(shape3),
        keys_float,
        values_float,
        log_decay,
        input_gate,
        regularizer,
        gram_prefix,
        cross_prefix,
    )
    return (attention, mesa_out.astype(jnp.bfloat16))


CHUNK = 128
WAYS = 4
BF16 = jnp.bfloat16
F32 = jnp.float32
NT = (((1,), (1,)), ((), ()))
TN = (((0,), (0,)), ((), ()))


def dot(a, b, dims=None):
    if dims is None:
        return jnp.dot(a, b, preferred_element_type=F32)
    return lax.dot_general(a, b, dims, preferred_element_type=F32)


def two_terms(a):
    high = a.astype(BF16)
    low = (a - high.astype(F32)).astype(BF16)
    return jnp.concatenate([high, low], axis=1)


def attend_block(q_ref, k_ref, v_ref, out_ref, i, first, count, rows, banded):
    scale = math.log2(math.e) / math.sqrt(q_ref.shape[1])
    queries = q_ref[pl.ds(pl.multiple_of(i * rows, rows), rows), :]
    base = pl.multiple_of(first * rows, rows)
    row = lax.broadcasted_iota(jnp.int32, (rows, rows), 0)
    col = lax.broadcasted_iota(jnp.int32, (rows, rows), 1)
    scores, top = [], None
    for j in range(count):
        s = dot(queries, k_ref[pl.ds(base + j * rows, rows), :], NT)
        if banded and j == 0:
            s = jnp.where(row - col + (count - 1) * rows < WINDOW, s, masked_score)
        if j == count - 1 or (not banded and j == count - 2):
            s = jnp.where(row - col + (i - first - j) * rows >= 0, s, masked_score)
        scores.append(s)
        top = s if top is None else jnp.maximum(top, s)
    top = jnp.max(top, axis=1, keepdims=True)
    total, weights = None, []
    for s in scores:
        w = jnp.exp2((s - top) * scale)
        total = w if total is None else total + w
        weights.append(w.astype(BF16))
    total = jnp.sum(total, axis=1, keepdims=True)
    summed = dot(
        jnp.concatenate(weights, axis=1), v_ref[pl.ds(base, count * rows), :]
    )
    out_ref[pl.ds(pl.multiple_of(i * rows, rows), rows), :] = (summed / total).astype(BF16)


def attend_all(q_ref, k_ref, v_ref, out_ref, rows, order, done):
    blocks = q_ref.shape[0] // rows
    reach = WINDOW // rows
    early = min(reach, blocks)

    def one(t, carry):
        i = order(t)
        for low in range(0, early, 2):
            high = min(low + 2, early)

            @pl.when((i >= low) & (i < high))
            def _(high=high):
                attend_block(q_ref, k_ref, v_ref, out_ref, i, 0, high, rows, False)

        if blocks > reach:

            @pl.when(i >= reach)
            def _():
                attend_block(q_ref, k_ref, v_ref, out_ref, i, i - reach, reach + 1, rows, True)

        done(i)
        return carry

    lax.fori_loop(0, blocks, one, 0)


def flat(c, per):
    return c[0] * per + c[1]


def span(c, per):
    return pl.ds(pl.multiple_of(flat(c, per) * CHUNK, CHUNK), CHUNK)


def chunk_ids(g, per, ways=WAYS):
    slabs = ways // per
    return [(g * slabs + w // per, w % per) for w in range(ways)]


def column_form(row):
    return jnp.transpose(jnp.broadcast_to(row, (CHUNK, CHUNK)))


def rates_of(rates_ref, c):
    slab, place = c
    per = rates_ref.shape[1] // 4
    return rates_ref[slab, place : place + 1, :], rates_ref[slab, per + place : per + place + 1, :]


def tail_keys(k_ref, rates_ref, c, per):
    cum, gate = rates_of(rates_ref, c)
    weight = column_form(jnp.exp(cum[:, CHUNK - 1 :] - cum) * gate)
    keys = k_ref[span(c, per), :]
    return (keys.astype(F32) * weight).astype(BF16), jnp.exp(cum[:, CHUNK - 1 :])


def mix_of(rates_ref, c):
    cum, gate = rates_of(rates_ref, c)
    col = column_form(cum)
    shape = (CHUNK, CHUNK)
    causal = lax.broadcasted_iota(jnp.int32, shape, 0) >= lax.broadcasted_iota(
        jnp.int32, shape, 1
    )
    mix = jnp.exp(jnp.where(causal, col - cum, masked_score)) * gate
    return mix, jnp.exp(col)


def gram_states(k_ref, other_ref, rates_ref, starts_ref):
    per = rates_ref.shape[1] // 4
    chunks = rates_ref.shape[0] * per

    def step(g, state):
        for c in chunk_ids(g, per):
            starts_ref[flat(c, per)] = state.astype(BF16)
            keys, end = tail_keys(k_ref, rates_ref, c, per)
            state = end * state + dot(keys, other_ref[span(c, per), :], TN)
        return state

    lax.fori_loop(0, chunks // WAYS, step, jnp.zeros((CHUNK, CHUNK), F32))


def solve_all(q_ref, k_ref, rates_ref, ridge_ref, gram_ref, x_ref):
    ridge = ridge_ref
    per = rates_ref.shape[1] // 4
    chunks = rates_ref.shape[0] * per

    def group(g, carry):
        ids = chunk_ids(g, per)
        mixes = [mix_of(rates_ref, c) for c in ids]
        keys = [k_ref[span(c, per), :] for c in ids]
        grams = [gram_ref[flat(c, per)] for c in ids]
        sides = [
            jnp.concatenate(
                [jnp.concatenate([a, a], axis=1), jnp.concatenate([k, k], axis=1)], axis=0
            )
            for a, k in zip(grams, keys)
        ]
        stacks = [jnp.concatenate([k, k], axis=0) for k in keys]
        state = []
        for c in ids:
            q = q_ref[span(c, per), :].astype(F32)
            state.append((jnp.zeros_like(q), q, q, jnp.sum(q * q, axis=1, keepdims=True)))

        def sweep(n, state):
            both = [dot(two_terms(s[2]), side, NT) for s, side in zip(state, sides)]
            local = [
                dot(two_terms(m[0] * b[:, CHUNK:]), k) for m, b, k in zip(mixes, both, stacks)
            ]
            out = []
            for (x, r, p, rr), b, l, m in zip(state, both, local, mixes):
                a = m[1] * b[:, :CHUNK] + l + ridge * p
                alpha = rr / (jnp.sum(p * a, axis=1, keepdims=True) + 1e-6)
                x = x + alpha * p
                r = r - alpha * a
                new = jnp.sum(r * r, axis=1, keepdims=True)
                p = r + (new / (rr + 1e-6)) * p
                out.append((x, r, p, new))
            return tuple(out)

        state = lax.fori_loop(0, CG_ITERS, sweep, tuple(state))
        for c, s in zip(ids, state):
            x_ref[span(c, per), :] = s[0]
        return carry

    lax.fori_loop(0, chunks // WAYS, group, 0)


def read_out(k_ref, v_ref, rates_ref, cross_ref, x_ref, out_ref, slab):
    per = rates_ref.shape[1] // 4
    for c in chunk_ids(slab, per, per):
        mix, start = mix_of(rates_ref, c)
        keys, values, cross = k_ref[span(c, per), :], v_ref[span(c, per), :], cross_ref[flat(c, per)]
        x = two_terms(x_ref[span(c, per), :])
        products = dot(x, jnp.concatenate([keys, keys], axis=1), NT)
        rows = start * dot(x, jnp.concatenate([cross, cross], axis=0))
        rows = rows + dot(two_terms(mix * products), jnp.concatenate([values, values], axis=0))
        out_ref[span(c, per), :] = rows.astype(BF16)


def head_kernel(n, *refs):
    ins, rates_in, ridge_in = refs[:5], refs[5], refs[6]
    results = refs[7:9]
    bufs, rates, homes = refs[9:14], refs[14], refs[15:17]
    gram, cross, x = refs[17:20]
    send, recv, own = refs[20:23]
    q, k, v, mk, mq = bufs
    att, out = homes
    rows, size = ins[0].shape[0], ridge_in.shape[1]
    group, me = lax.axis_index("groups"), lax.axis_index("seq")

    def row_block(ref, s):
        return ref.at[pl.ds(pl.multiple_of(s * rows, rows), rows), :]

    def col_block(ref, h):
        return ref.at[:, pl.ds(pl.multiple_of(h * size, size), size)]

    def ends(a, source, target):
        if a < 5:
            return col_block(ins[a], target), row_block(bufs[a], source)
        if a == 5:
            return rates_in.at[target], rates.at[source]
        return row_block(homes[a - 6], target), col_block(results[a - 6], source)

    def remote(a, source, target, peer):
        src, dst = ends(a, source, target)
        return pltpu.make_async_remote_copy(
            src_ref=src,
            dst_ref=dst,
            send_sem=send.at[a, target],
            recv_sem=recv.at[a, source],
            device_id=(group, peer),
            device_id_type=pl.DeviceIdType.MESH,
        )

    def local(a):
        src, dst = ends(a, me, me)
        return pltpu.make_async_copy(src, dst, own.at[a])

    def other(t):
        return lax.rem(me + t, n)

    def over_peers(act):
        def one(t, carry):
            act(other(t))
            return carry

        lax.fori_loop(1, n, one, 0)

    def arrive(a):
        over_peers(lambda peer: remote(a, peer, me, peer).wait_recv())
        local(a).wait()

    def give(a, slab):
        @pl.when(slab != me)
        def _():
            remote(a, me, slab, slab).start()

        @pl.when(slab == me)
        def _():
            local(a).start()

    barrier = pltpu.get_barrier_semaphore()
    over_peers(
        lambda peer: pl.semaphore_signal(
            barrier, inc=1, device_id=(group, peer), device_id_type=pl.DeviceIdType.MESH
        )
    )
    pl.semaphore_wait(barrier, n - 1)
    for a in SEND_ORDER:
        over_peers(lambda peer: remote(a, me, peer, peer).start())
        local(a).start()

    for a in (5, 3, 4):
        arrive(a)
    gram_states(mk, mk, rates, gram)
    solve_all(mq, mk, rates, ridge_in[pl.ds(me, 1), :], gram, x)
    for a in (0, 1, 2):
        arrive(a)
    attend_all(q, k, v, att, rows, lambda t: other(t + 1), lambda i: give(6, i))
    gram_states(mk, att, rates, cross)

    def slab_out(t, carry):
        slab = other(t + 1)
        read_out(mk, att, rates, cross, x, out, slab)
        give(7, slab)
        return carry

    lax.fori_loop(0, n, slab_out, 0)
    for a in (6, 7):
        arrive(a)
    for a in range(8):
        over_peers(lambda peer: remote(a, me, peer, peer).wait_send())


SEND_ORDER = (5, 3, 4, 0, 1, 2)


def head_body(
    attn_query, attn_key, attn_value, mesa_query, mesa_key, log_decay, input_gate, regularizer
):
    rows = attn_query.shape[0]
    heads, size = regularizer.shape
    devices = lax.axis_size("seq")
    tokens = rows * devices
    per, chunks = rows // CHUNK, tokens // CHUNK
    cum = jnp.cumsum(log_decay.reshape(per, CHUNK, heads), axis=1)
    rates = jnp.concatenate([cum, input_gate.reshape(per, CHUNK, heads)], axis=0)
    rates = jnp.pad(jnp.transpose(rates, (2, 0, 1)), ((0, 0), (0, 2 * per), (0, 0)))
    slab = jax.ShapeDtypeStruct((rows, heads * size), BF16)
    vmem = pl.BlockSpec(memory_space=pltpu.VMEM)
    anywhere = pl.BlockSpec(memory_space=pl.ANY)
    return pl.pallas_call(
        functools.partial(head_kernel, devices),
        out_shape=(slab, slab),
        in_specs=[anywhere] * 5 + [vmem] * 2,
        out_specs=(anywhere, anywhere),
        scratch_shapes=[pltpu.VMEM((tokens, size), BF16)] * 5
        + [pltpu.VMEM((devices, 4 * per, CHUNK), F32)]
        + [pltpu.VMEM((tokens, size), BF16)] * 2
        + [pltpu.VMEM((chunks, size, size), BF16)] * 2
        + [
            pltpu.VMEM((tokens, size), F32),
            pltpu.SemaphoreType.DMA((8, devices)),
            pltpu.SemaphoreType.DMA((8, devices)),
            pltpu.SemaphoreType.DMA((8,)),
        ],
        compiler_params=pltpu.CompilerParams(
            collective_id=0, has_side_effects=True, vmem_limit_bytes=56 * 1024 * 1024
        ),
    )(attn_query, attn_key, attn_value, mesa_key, mesa_query, rates, regularizer)


def fits_heads(mesh, rows, heads, size):
    tokens = rows * mesh.shape["seq"]
    return (
        mesh.shape["seq"] == heads
        and size == CHUNK
        and WINDOW % rows == 0
        and rows % CHUNK == 0
        and WAYS % (rows // CHUNK) == 0
        and tokens % (CHUNK * WAYS) == 0
    )


def solution(mesh):
    spec = P(("groups", "seq"), None)

    def body(*args):
        heads, size = args[7].shape
        chosen = head_body if fits_heads(mesh, args[0].shape[0], heads, size) else slab_body
        return chosen(*args)

    return jax.shard_map(
        body,
        mesh=mesh,
        in_specs=(spec,) * 7 + (P(),),
        out_specs=(spec, spec),
        check_vma=False,
    )
```

```python
import jax
import jax.numpy as jnp
from jax import lax
from jax.experimental import pallas as pl
from jax.experimental.pallas import tpu as pltpu
from jax.sharding import PartitionSpec as P
import functools
import math

WINDOW = 2048
SPAN = 64
CG_ITERS = 8


exact_mode = lax.Precision.HIGHEST
masked_score = -1e30


def prefix(shard, axis, join, neutral):
    place = lax.axis_index(axis)
    gathered = jax.tree.map(
        lambda a, kind: lax.all_gather(a.astype(kind), axis), shard, (jnp.bfloat16, jnp.bfloat16)
    )
    state = jax.tree.map(lambda a, e: jnp.zeros_like(a) + jnp.asarray(e, a.dtype), shard, neutral)

    def one(lap, state):
        return join(
            state,
            jax.tree.map(
                lambda a, own: lax.dynamic_index_in_dim(a, lap, 0, False).astype(own.dtype),
                gathered,
                shard,
            ),
        )

    return lax.fori_loop(0, place, one, state)


def passed_along(value, axis, steps):
    count = lax.axis_size(axis)
    first, last = (max(0, -steps), min(count, count - steps))
    return lax.ppermute(value, axis, [(source, source + steps) for source in range(first, last)])


def span_update(states, inputs, ridge_diag):
    gram_start, cross_start = states
    queries, key_rows, value_rows, log_rates, gate_rows = inputs
    q_heads = jnp.transpose(queries, (1, 0, 2))
    k_heads = jnp.transpose(key_rows, (1, 0, 2))
    v_heads = jnp.transpose(value_rows, (1, 0, 2))
    cumulative = jnp.transpose(jnp.cumsum(log_rates, axis=0))
    length = cumulative.shape[1]
    causal = (jnp.arange(length)[:, None] >= jnp.arange(length)[None, :])[None]
    distance = cumulative[:, :, None] - cumulative[:, None, :]
    decay_mix = (
        jnp.where(causal, jnp.exp(jnp.where(causal, distance, 0.0)), 0.0)
        * jnp.transpose(gate_rows)[:, None, :]
    )
    start_scale = jnp.exp(cumulative)[:, :, None]
    iterate = jnp.zeros_like(q_heads)
    remain = q_heads
    search = q_heads
    norm_now = jnp.sum(remain * remain, axis=-1, keepdims=True)
    for sweep_index in range(CG_ITERS):
        carried = start_scale * jnp.einsum("hcd,hed->hce", search, gram_start, precision=exact_mode)
        operator_products = jnp.einsum("hjd,hid->hji", search, k_heads, precision=exact_mode)
        local_part = jnp.einsum(
            "hji,hid->hjd", decay_mix * operator_products, k_heads, precision=exact_mode
        )
        image_vec = carried + local_part + ridge_diag[:, None, :] * search
        step_size = norm_now / (jnp.sum(search * image_vec, axis=-1, keepdims=True) + 1e-06)
        iterate = iterate + step_size * search
        remain = remain - step_size * image_vec
        norm_next = jnp.sum(remain * remain, axis=-1, keepdims=True)
        search = remain + norm_next / (norm_now + 1e-06) * search
        norm_now = norm_next
    products = jnp.einsum("hjd,hid->hji", iterate, k_heads, precision=exact_mode)
    mesa_rows = start_scale * jnp.einsum("hje,hde->hjd", iterate, cross_start, precision=exact_mode)
    mesa_rows = mesa_rows + jnp.einsum(
        "hji,hid->hjd", decay_mix * products, v_heads, precision=exact_mode
    )
    tail_weight = (jnp.exp(cumulative[:, -1:] - cumulative) * jnp.transpose(gate_rows))[:, :, None]
    end_scale = jnp.exp(cumulative[:, -1])[:, None, None]
    gram_end = end_scale * gram_start + jnp.einsum(
        "hid,hie->hde", k_heads * tail_weight, k_heads, precision=exact_mode
    )
    cross_end = end_scale * cross_start + jnp.einsum(
        "hid,hie->hde", v_heads * tail_weight, k_heads, precision=exact_mode
    )
    return ((gram_end, cross_end), jnp.transpose(mesa_rows, (1, 0, 2)))


def mesa_pass(
    queries, key_rows, value_rows, log_rates, gate_rows, ridge_diag, gram_start, cross_start
):
    row_total = queries.shape[0]
    span_count = row_total // SPAN

    def shaped(array_in):
        return array_in.reshape((span_count, SPAN) + array_in.shape[1:])

    def advance(states, inputs):
        return span_update(states, inputs, ridge_diag)

    finished, outputs = lax.scan(
        advance,
        (gram_start, cross_start),
        (
            shaped(queries),
            shaped(key_rows),
            shaped(value_rows),
            shaped(log_rates),
            shaped(gate_rows),
        ),
    )
    return outputs.reshape(row_total, -1)


def fold_block(state_now, queries, key_value, query_first, key_first):
    running_max, running_sum, weighted = state_now
    row_count, head_count, head_size = queries.shape
    key_rows = key_value[0].reshape(-1, head_count, head_size)
    value_rows = key_value[1].reshape(-1, head_count, head_size)
    scores = jnp.einsum(
        "qhd,khd->hqk", queries, key_rows, preferred_element_type=jnp.float32
    ) * head_size ** (-0.5)
    query_pos = query_first + jnp.arange(row_count, dtype=jnp.int32)[:, None]
    key_pos = key_first + jnp.arange(key_rows.shape[0], dtype=jnp.int32)[None, :]
    distance = query_pos - key_pos
    inside = ((distance >= 0) & (distance < WINDOW) & (key_pos >= 0))[None]
    scores = jnp.where(inside, scores, masked_score)
    new_max = jnp.maximum(running_max, jnp.max(scores, axis=-1))
    weights = jnp.exp(scores - new_max[:, :, None]) * inside.astype(jnp.float32)
    rescale = jnp.exp(running_max - new_max)
    running_sum = running_sum * rescale + jnp.sum(weights, axis=-1)
    weighted = weighted * rescale[:, :, None] + jnp.einsum(
        "hqk,khd->hqd", weights.astype(jnp.bfloat16), value_rows, preferred_element_type=jnp.float32
    )
    return (new_max, running_sum, weighted)


def combine_pair(earlier, later):
    return (earlier[0] + later[0], jnp.exp(later[0])[:, None, None] * earlier[1] + later[1])


def slab_body(
    attn_query, attn_key, attn_value, mesa_query, mesa_key, log_decay, input_gate, regularizer
):
    row_count = attn_query.shape[0]
    head_count, head_size = regularizer.shape
    shape3 = (row_count, head_count, head_size)
    slab_first = lax.axis_index("seq") * row_count
    keys_float = mesa_key.astype(jnp.float32).reshape(shape3)
    slab_log = jnp.sum(log_decay, axis=0)
    tail_log = slab_log[None, :] - jnp.cumsum(log_decay, axis=0)
    weight_rows = (jnp.exp(tail_log) * input_gate)[:, :, None]
    gram_local = jnp.einsum(
        "lhd,lhe->hde", keys_float * weight_rows, keys_float, precision=exact_mode
    )
    zero_log = jnp.zeros_like(slab_log)
    zero_state = jnp.zeros_like(gram_local)
    gram_prefix = prefix((slab_log, gram_local), "seq", combine_pair, (zero_log, zero_state))[1]
    queries = attn_query.reshape(shape3)
    key_value = jnp.stack([attn_key, attn_value])
    state_now = (
        jnp.full((head_count, row_count), masked_score, jnp.float32),
        jnp.zeros((head_count, row_count), jnp.float32),
        jnp.zeros((head_count, row_count, head_size), jnp.float32),
    )
    state_now = fold_block(state_now, queries, key_value, slab_first, slab_first)
    reach = -(-WINDOW // row_count)
    moving = key_value
    for hop_index in range(1, reach + 1):
        moving = passed_along(moving, "seq", 1)
        state_now = fold_block(
            state_now, queries, moving, slab_first, slab_first - hop_index * row_count
        )
    normed = state_now[2] / state_now[1][:, :, None]
    attention = jnp.transpose(normed, (1, 0, 2)).reshape(row_count, -1).astype(jnp.bfloat16)
    values_float = attention.astype(jnp.float32).reshape(shape3)
    cross_local = jnp.einsum(
        "lhd,lhe->hde", values_float * weight_rows, keys_float, precision=exact_mode
    )
    cross_prefix = prefix((slab_log, cross_local), "seq", combine_pair, (zero_log, zero_state))[1]
    mesa_out = mesa_pass(
        mesa_query.astype(jnp.float32).reshape(shape3),
        keys_float,
        values_float,
        log_decay,
        input_gate,
        regularizer,
        gram_prefix,
        cross_prefix,
    )
    return (attention, mesa_out.astype(jnp.bfloat16))


CHUNK = 128
WAYS = 4
BF16 = jnp.bfloat16
F32 = jnp.float32
NT = (((1,), (1,)), ((), ()))
TN = (((0,), (0,)), ((), ()))


def dot(a, b, dims=None):
    if dims is None:
        return jnp.dot(a, b, preferred_element_type=F32)
    return lax.dot_general(a, b, dims, preferred_element_type=F32)


def two_terms(a):
    high = a.astype(BF16)
    low = (a - high.astype(F32)).astype(BF16)
    return jnp.concatenate([high, low], axis=1)


def attend_block(q_ref, k_ref, v_ref, out_ref, i, first, count, rows, banded):
    scale = math.log2(math.e) / math.sqrt(q_ref.shape[1])
    queries = q_ref[pl.ds(pl.multiple_of(i * rows, rows), rows), :]
    base = pl.multiple_of(first * rows, rows)
    row = lax.broadcasted_iota(jnp.int32, (rows, rows), 0)
    col = lax.broadcasted_iota(jnp.int32, (rows, rows), 1)
    scores, top = [], None
    for j in range(count):
        s = dot(queries, k_ref[pl.ds(base + j * rows, rows), :], NT)
        if banded and j == 0:
            s = jnp.where(row - col + (count - 1) * rows < WINDOW, s, masked_score)
        if j == count - 1 or (not banded and j == count - 2):
            s = jnp.where(row - col + (i - first - j) * rows >= 0, s, masked_score)
        scores.append(s)
        top = s if top is None else jnp.maximum(top, s)
    top = jnp.max(top, axis=1, keepdims=True)
    total, weights = None, []
    for s in scores:
        w = jnp.exp2((s - top) * scale)
        total = w if total is None else total + w
        weights.append(w.astype(BF16))
    total = jnp.sum(total, axis=1, keepdims=True)
    summed = dot(
        jnp.concatenate(weights, axis=1), v_ref[pl.ds(base, count * rows), :]
    )
    out_ref[pl.ds(pl.multiple_of(i * rows, rows), rows), :] = (summed / total).astype(BF16)


def attend_all(q_ref, k_ref, v_ref, out_ref, rows, order, done):
    blocks = q_ref.shape[0] // rows
    reach = WINDOW // rows
    early = min(reach, blocks)

    def one(t, carry):
        i = order(t)
        for low in range(0, early, 2):
            high = min(low + 2, early)

            @pl.when((i >= low) & (i < high))
            def _(high=high):
                attend_block(q_ref, k_ref, v_ref, out_ref, i, 0, high, rows, False)

        if blocks > reach:

            @pl.when(i >= reach)
            def _():
                attend_block(q_ref, k_ref, v_ref, out_ref, i, i - reach, reach + 1, rows, True)

        done(i)
        return carry

    lax.fori_loop(0, blocks, one, 0)


def flat(c, per):
    return c[0] * per + c[1]


def span(c, per):
    return pl.ds(pl.multiple_of(flat(c, per) * CHUNK, CHUNK), CHUNK)


def chunk_ids(g, per, ways=WAYS):
    slabs = ways // per
    return [(g * slabs + w // per, w % per) for w in range(ways)]


def column_form(row):
    return jnp.transpose(jnp.broadcast_to(row, (CHUNK, CHUNK)))


def rates_of(rates_ref, c):
    slab, place = c
    per = rates_ref.shape[1] // 4
    return rates_ref[slab, place : place + 1, :], rates_ref[slab, per + place : per + place + 1, :]


def tail_keys(k_ref, rates_ref, c, per):
    cum, gate = rates_of(rates_ref, c)
    weight = column_form(jnp.exp(cum[:, CHUNK - 1 :] - cum) * gate)
    keys = k_ref[span(c, per), :]
    return (keys.astype(F32) * weight).astype(BF16), jnp.exp(cum[:, CHUNK - 1 :])


def mix_of(rates_ref, c):
    cum, gate = rates_of(rates_ref, c)
    col = column_form(cum)
    shape = (CHUNK, CHUNK)
    causal = lax.broadcasted_iota(jnp.int32, shape, 0) >= lax.broadcasted_iota(
        jnp.int32, shape, 1
    )
    mix = jnp.exp(jnp.where(causal, col - cum, masked_score)) * gate
    return mix, jnp.exp(col)


def gram_states(k_ref, other_ref, rates_ref, starts_ref):
    per = rates_ref.shape[1] // 4
    chunks = rates_ref.shape[0] * per

    def step(g, state):
        for c in chunk_ids(g, per):
            starts_ref[flat(c, per)] = state.astype(BF16)
            keys, end = tail_keys(k_ref, rates_ref, c, per)
            state = end * state + dot(keys, other_ref[span(c, per), :], TN)
        return state

    lax.fori_loop(0, chunks // WAYS, step, jnp.zeros((CHUNK, CHUNK), F32))


def solve_all(q_ref, k_ref, rates_ref, ridge_ref, gram_ref, x_ref):
    ridge = ridge_ref
    per = rates_ref.shape[1] // 4
    chunks = rates_ref.shape[0] * per

    def group(g, carry):
        ids = chunk_ids(g, per)
        mixes = [mix_of(rates_ref, c) for c in ids]
        keys = [k_ref[span(c, per), :] for c in ids]
        grams = [gram_ref[flat(c, per)] for c in ids]
        sides = [
            jnp.concatenate(
                [jnp.concatenate([a, a], axis=1), jnp.concatenate([k, k], axis=1)], axis=0
            )
            for a, k in zip(grams, keys)
        ]
        stacks = [jnp.concatenate([k, k], axis=0) for k in keys]
        state = []
        for c in ids:
            q = q_ref[span(c, per), :].astype(F32)
            state.append((jnp.zeros_like(q), q, q, jnp.sum(q * q, axis=1, keepdims=True)))

        def sweep(n, state):
            both = [dot(two_terms(s[2]), side, NT) for s, side in zip(state, sides)]
            local = [
                dot(two_terms(m[0] * b[:, CHUNK:]), k) for m, b, k in zip(mixes, both, stacks)
            ]
            out = []
            for (x, r, p, rr), b, l, m in zip(state, both, local, mixes):
                a = m[1] * b[:, :CHUNK] + l + ridge * p
                alpha = rr / (jnp.sum(p * a, axis=1, keepdims=True) + 1e-6)
                x = x + alpha * p
                r = r - alpha * a
                new = jnp.sum(r * r, axis=1, keepdims=True)
                p = r + (new / (rr + 1e-6)) * p
                out.append((x, r, p, new))
            return tuple(out)

        state = lax.fori_loop(0, CG_ITERS, sweep, tuple(state))
        for w, (c, s) in enumerate(zip(ids, state)):
            mix, start = mixes[w]
            products = dot(two_terms(s[0]), jnp.concatenate([keys[w]] * 2, axis=1), NT)
            x_ref[span(c, per), :] = jnp.concatenate(
                [two_terms(start * s[0]), two_terms(mix * products)], axis=1
            )
        return carry

    lax.fori_loop(0, chunks // WAYS, group, 0)


def read_out(k_ref, v_ref, rates_ref, cross_ref, x_ref, out_ref, slab):
    per = rates_ref.shape[1] // 4
    for c in chunk_ids(slab, per, per):
        values, cross = v_ref[span(c, per), :], cross_ref[flat(c, per)]
        rows = dot(
            x_ref[span(c, per), :], jnp.concatenate([cross, cross, values, values], axis=0)
        )
        out_ref[span(c, per), :] = rows.astype(BF16)


def head_kernel(n, *refs):
    ins, rates_in, ridge_in = refs[:5], refs[5], refs[6]
    results = refs[7:9]
    bufs, rates, homes = refs[9:14], refs[14], refs[15:17]
    gram, cross, x = refs[17:20]
    send, recv, own = refs[20:23]
    q, k, v, mk, mq = bufs
    att, out = homes
    rows, size = ins[0].shape[0], ridge_in.shape[1]
    group, me = lax.axis_index("groups"), lax.axis_index("seq")

    def row_block(ref, s):
        return ref.at[pl.ds(pl.multiple_of(s * rows, rows), rows), :]

    def col_block(ref, h):
        return ref.at[:, pl.ds(pl.multiple_of(h * size, size), size)]

    def ends(a, source, target):
        if a < 5:
            return col_block(ins[a], target), row_block(bufs[a], source)
        if a == 5:
            return rates_in.at[target], rates.at[source]
        return row_block(homes[a - 6], target), col_block(results[a - 6], source)

    def remote(a, source, target, peer):
        src, dst = ends(a, source, target)
        return pltpu.make_async_remote_copy(
            src_ref=src,
            dst_ref=dst,
            send_sem=send.at[a, target],
            recv_sem=recv.at[a, source],
            device_id=(group, peer),
            device_id_type=pl.DeviceIdType.MESH,
        )

    def local(a):
        src, dst = ends(a, me, me)
        return pltpu.make_async_copy(src, dst, own.at[a])

    def other(t):
        return lax.rem(me + t, n)

    def over_peers(act):
        def one(t, carry):
            act(other(t))
            return carry

        lax.fori_loop(1, n, one, 0)

    def arrive(a):
        over_peers(lambda peer: remote(a, peer, me, peer).wait_recv())
        local(a).wait()

    def give(a, slab):
        @pl.when(slab != me)
        def _():
            remote(a, me, slab, slab).start()

        @pl.when(slab == me)
        def _():
            local(a).start()

    barrier = pltpu.get_barrier_semaphore()
    over_peers(
        lambda peer: pl.semaphore_signal(
            barrier, inc=1, device_id=(group, peer), device_id_type=pl.DeviceIdType.MESH
        )
    )
    pl.semaphore_wait(barrier, n - 1)
    for a in SEND_ORDER:
        over_peers(lambda peer: remote(a, me, peer, peer).start())
        local(a).start()

    for a in (5, 3, 4):
        arrive(a)
    gram_states(mk, mk, rates, gram)
    solve_all(mq, mk, rates, ridge_in[pl.ds(me, 1), :], gram, x)
    for a in (0, 1, 2):
        arrive(a)
    attend_all(q, k, v, att, rows, lambda t: other(t + 1), lambda i: give(6, i))
    gram_states(mk, att, rates, cross)

    def slab_out(t, carry):
        slab = other(t + 1)
        read_out(mk, att, rates, cross, x, out, slab)
        give(7, slab)
        return carry

    lax.fori_loop(0, n, slab_out, 0)
    for a in (6, 7):
        arrive(a)
    for a in range(8):
        over_peers(lambda peer: remote(a, me, peer, peer).wait_send())


SEND_ORDER = (5, 3, 4, 0, 1, 2)


def head_body(
    attn_query, attn_key, attn_value, mesa_query, mesa_key, log_decay, input_gate, regularizer
):
    rows = attn_query.shape[0]
    heads, size = regularizer.shape
    devices = lax.axis_size("seq")
    tokens = rows * devices
    per, chunks = rows // CHUNK, tokens // CHUNK
    cum = jnp.cumsum(log_decay.reshape(per, CHUNK, heads), axis=1)
    rates = jnp.concatenate([cum, input_gate.reshape(per, CHUNK, heads)], axis=0)
    rates = jnp.pad(jnp.transpose(rates, (2, 0, 1)), ((0, 0), (0, 2 * per), (0, 0)))
    slab = jax.ShapeDtypeStruct((rows, heads * size), BF16)
    vmem = pl.BlockSpec(memory_space=pltpu.VMEM)
    anywhere = pl.BlockSpec(memory_space=pl.ANY)
    return pl.pallas_call(
        functools.partial(head_kernel, devices),
        out_shape=(slab, slab),
        in_specs=[anywhere] * 5 + [vmem] * 2,
        out_specs=(anywhere, anywhere),
        scratch_shapes=[pltpu.VMEM((tokens, size), BF16)] * 5
        + [pltpu.VMEM((devices, 4 * per, CHUNK), F32)]
        + [pltpu.VMEM((tokens, size), BF16)] * 2
        + [pltpu.VMEM((chunks, size, size), BF16)] * 2
        + [
            pltpu.VMEM((tokens, 4 * size), BF16),
            pltpu.SemaphoreType.DMA((8, devices)),
            pltpu.SemaphoreType.DMA((8, devices)),
            pltpu.SemaphoreType.DMA((8,)),
        ],
        compiler_params=pltpu.CompilerParams(
            collective_id=0, has_side_effects=True, vmem_limit_bytes=56 * 1024 * 1024
        ),
    )(attn_query, attn_key, attn_value, mesa_key, mesa_query, rates, regularizer)


def fits_heads(mesh, rows, heads, size):
    tokens = rows * mesh.shape["seq"]
    return (
        mesh.shape["seq"] == heads
        and size == CHUNK
        and WINDOW % rows == 0
        and rows % CHUNK == 0
        and WAYS % (rows // CHUNK) == 0
        and tokens % (CHUNK * WAYS) == 0
    )


def solution(mesh):
    spec = P(("groups", "seq"), None)

    def body(*args):
        heads, size = args[7].shape
        chosen = head_body if fits_heads(mesh, args[0].shape[0], heads, size) else slab_body
        return chosen(*args)

    return jax.shard_map(
        body,
        mesh=mesh,
        in_specs=(spec,) * 7 + (P(),),
        out_specs=(spec, spec),
        check_vma=False,
    )
```
